32 devices in a mesh: rep: 1, r: 8 (over y, z), s: 4 (over x, core).
Axes of the slice: x: 2, y: 2, z: 4, core: 2. Of those that a mesh axis runs over, the one named last changes fastest.
Arguments:
- x: bfloat16 [32, 4096, 640], P(('rep', 'r', 's'))
- dy: bfloat16 [32, 4096, 640], P(('rep', 'r', 's'))
- w_gate: bfloat16 [2, 640, 2176], P(None, 's')
- w_up: bfloat16 [2, 640, 2176], P(None, 's')
- w_down: bfloat16 [2, 2176, 640], P(None, 's')
Outputs:
- output 1: bfloat16 [32, 4096, 640], P(('rep', 'r', 's'))
- output 2: bfloat16 [2, 640, 2176], P('rep', 's')
- output 3: bfloat16 [2, 640, 2176], P('rep', 's')
- output 4: bfloat16 [2, 2176, 640], P('rep', 's')
All inputs are finite; a program needn't handle non-finite values.
Results may differ from the reference program's by a relative error of at most 0.018.
Values are sent between devices in bfloat16 or wider.
A program may use at most 2 GiB of HBM per device.

```python
import jax
import jax.numpy as jnp
from jax import lax

SEQUENCES = 32
TOKENS = 4096
D = 640
FF = 2176
LAYERS = 2
NAMES = ("w_gate", "w_up", "w_down")
SHAPES = {"w_gate": (LAYERS, D, FF), "w_up": (LAYERS, D, FF), "w_down": (LAYERS, FF, D)}


def bump(key, n, height):
    away = (jnp.arange(n, dtype=jnp.int32) - jax.random.randint(key, (), 0, n, jnp.int32)) % n
    return jnp.where(away < n // 8, height, 1.0)


def together(key, own, strength):
    shared = jax.random.normal(key, own.shape[1:], jnp.float32)
    return (own + strength * shared) * lax.rsqrt(1 + strength * strength)


def setup_inputs(seed: int = 0, part: int = 0) -> dict:
    kx, kdy, ka, kb, kz, kf, kh, kl, *kw = jax.random.split(jax.random.key(seed), 8 + len(NAMES))
    kx, kdy, ka, kb = (jax.random.fold_in(k, part) for k in (kx, kdy, ka, kb))
    shape = (SEQUENCES, TOKENS, D)
    much_x, much_dy = jax.random.uniform(kz, (2,), jnp.float32, 0.0, 1.0)
    layers = 2.0 ** jax.random.uniform(kl, (LAYERS, 1, 1), jnp.float32, -1.0, 1.0)
    x = together(ka, jax.random.normal(kx, shape, jnp.float32), much_x) * bump(kf, D, 4.0)
    dy = together(kb, jax.random.normal(kdy, shape, jnp.float32), much_dy)
    drawn = {"x": x.astype(jnp.bfloat16), "dy": (dy * (SEQUENCES * TOKENS) ** -0.5).astype(jnp.bfloat16)}
    for key, name in zip(kw, NAMES, strict=True):
        w = jax.random.normal(key, SHAPES[name], jnp.float32) * SHAPES[name][1] ** -0.5
        drawn[name] = (w * {"w_gate": 1.0, "w_up": bump(kh, FF, 4.0), "w_down": layers}[name]).astype(jnp.bfloat16)
    return drawn


def matmul(a, w):
    return jnp.dot(a, w, preferred_element_type=jnp.float32).astype(jnp.bfloat16)


def normed(h):
    wide = h.astype(jnp.float32)
    scale = lax.rsqrt(jnp.mean(wide**2, -1, keepdims=True) + 1e-6)
    return (wide * scale).astype(jnp.bfloat16)


def layer(h, w):
    a = normed(h)
    gate = jnp.dot(a, w["w_gate"], preferred_element_type=jnp.float32)
    up = jnp.dot(a, w["w_up"], preferred_element_type=jnp.float32)
    return h + matmul((jax.nn.silu(gate) * up).astype(jnp.bfloat16), w["w_down"])


def stack(weights, h):
    return lax.scan(lambda h, w: (layer(h, w), None), h, weights)[0]


def reference(x, dy, w_gate, w_up, w_down):
    weights = dict(zip(NAMES, (w_gate, w_up, w_down), strict=True))

    def take(so_far, sequence):
        h, by_y = sequence
        _, back = jax.vjp(stack, weights, h)
        by_weights, by_h = back(by_y)
        return jax.tree.map(lambda total, term: total + term.astype(jnp.float32), so_far, by_weights), by_h

    none_yet = {name: jnp.zeros(w.shape, jnp.float32) for name, w in weights.items()}
    by_weights, by_x = lax.scan(take, none_yet, (x, dy))
    return (by_x, *(by_weights[name].astype(jnp.bfloat16) for name in NAMES))
```

```python
import functools
import jax
import jax.numpy as jnp
from jax import lax
from jax.experimental import pallas as pl
from jax.experimental.pallas import tpu as pltpu
from jax.sharding import PartitionSpec as P

T, D, F, EPS = 4096, 640, 2176, 1e-6
BF, F32 = jnp.bfloat16, jnp.float32
TT = 512
CH = [(i * 256, 256) for i in range(8)] + [(2048, 128)]
ANY = pl.BlockSpec(memory_space=pl.ANY)
NT = (((1,), (1,)), ((), ()))


def dot(a, b):
    return jnp.dot(a, b, preferred_element_type=F32)


def dot_nt(a, b):
    return lax.dot_general(a, b, NT, preferred_element_type=F32)


def params(limit=60):
    return pltpu.CompilerParams(vmem_limit_bytes=limit * 2**20)


def cost(flops, nbytes):
    return pl.CostEstimate(flops=int(flops), bytes_accessed=int(nbytes), transcendentals=0)


def norm_of(h):
    wide = h.astype(F32)
    scale = lax.rsqrt(jnp.mean(wide * wide, -1, keepdims=True) + EPS)
    return wide, scale


def sigmoid(g):
    return 1.0 / (1.0 + jnp.exp(-g))


def grads_of(g, u, dact):
    sig = sigmoid(g)
    silu = g * sig
    act = (silu * u).astype(BF)
    dup = dact * silu
    dgate = dact * u * (sig + silu * (1.0 - sig))
    return act, dgate.astype(BF), dup.astype(BF)


def norm_back(da, wide, scale, dy):
    da = da.astype(BF).astype(F32)
    inner = jnp.mean(da * wide, -1, keepdims=True)
    dwide = scale * da - wide * (scale * scale * scale * inner)
    return (dy.astype(F32) + dwide.astype(BF).astype(F32)).astype(BF)


CORE, X, Z1, Z2, Y = range(5)
MESH = pl.DeviceIdType.MESH


def places():
    rep, r, s = lax.axis_index("rep"), lax.axis_index("r"), lax.axis_index("s")
    y, z, x, core = r // 4, r % 4, s // 2, s % 2
    at = lambda y, z, x, core: (rep, y * 4 + z, x * 2 + core)
    low, high = z % 2, z // 2
    partners = [
        at(y, z, x, 1 - core),
        at(y, z, 1 - x, core),
        at(y, high * 2 + 1 - low, x, core),
        at(y, (1 - high) * 2 + low, x, core),
        at(1 - y, z, x, core),
    ]
    return y, low, x, core, s, partners


def greet(partners):
    barrier = pltpu.get_barrier_semaphore()
    for partner in partners:
        pl.semaphore_signal(barrier, inc=1, device_id=partner, device_id_type=MESH)
    pl.semaphore_wait(barrier, len(partners))


def remote(src, dst, send, recv, partner):
    return pltpu.make_async_remote_copy(src_ref=src, dst_ref=dst, send_sem=send, recv_sem=recv, device_id=partner, device_id_type=MESH)


def k1(x_ref, wg, wu, wd, gate_ref, up_ref, act_ref, actt_ref, at_ref, og, ou, od, wgu, sg, su, sd, send, recv, local):
    i = pl.program_id(0)
    y, low, x, core, s, partners = places()
    tensors = [(w, o, stage, layer, rows) for layer in range(2) for w, o, stage, rows in ((wg, og, sg, 160), (wu, ou, su, 160), (wd, od, sd, 544))]

    def copy(k, kind):
        w, o, _, layer, rows = tensors[k]
        half = rows // 2
        across = jnp.bitwise_xor(s, 2)
        own = lambda n, at: o.at[layer, pl.ds(pl.multiple_of(at, 16), n)]
        if kind == 0:
            src, dst, partner = w.at[layer], own(rows, s * rows), CORE
        elif kind == 1:
            src, dst, partner = w.at[layer, pl.ds(pl.multiple_of(y * half, 16), half)], own(half, s * rows + y * half), X
        elif kind in (2, 3):
            src = own(half, across * rows + y * half)
            dst, partner = src, Y if kind == 2 else CORE
        else:
            src = own(half, across * rows + (1 - y) * half)
            dst, partner = src, CORE
        return remote(src, dst, send.at[k, kind], recv.at[k, kind], partners[partner])

    def stage_in(k):
        w, _, stage, layer, _ = tensors[k]
        return pltpu.make_async_copy(w.at[layer], stage.at[layer], local.at[k, 0])

    def stage_out(k):
        _, o, stage, layer, rows = tensors[k]
        return pltpu.make_async_copy(stage.at[layer], o.at[layer, pl.ds(pl.multiple_of(s * rows, 32), rows)], local.at[k, 1])

    def forward_x(k):
        copy(k, 1).wait_recv()
        copy(k, 2).start()
        copy(k, 3).start()

    def forward_y(k):
        copy(k, 2).wait_recv()
        copy(k, 4).start()

    @pl.when(i == 0)
    def _():
        greet([partners[CORE], partners[X], partners[Y]])
        copy(0, 1).start()
        copy(1, 1).start()
        copy(0, 0).start()
        copy(1, 0).start()
        for k in range(6):
            stage_in(k).start()
        for k in range(6):
            stage_in(k).wait()
            stage_out(k).start()
        forward_x(0)
        copy(2, 1).start()
        forward_x(1)
        for k in range(3, 6):
            copy(k, 1).start()
        forward_y(0)
        forward_y(1)
        for k in range(2):
            stage_out(k).wait()
            for kind in (0, 3, 4):
                copy(k, kind).wait_recv()
        loads = [pltpu.make_async_copy(o.at[0], wgu.at[:, pl.ds(c, F)], local.at[c // F, 0]) for o, c in ((og, 0), (ou, F))]
        for load in loads:
            load.start()
        for k in range(2, 6):
            copy(k, 0).start()
        for load in loads:
            load.wait()

    for when, todo in {1: ((forward_x, 2),), 3: ((forward_x, 3), (forward_y, 2)), 4: ((forward_x, 4), (forward_y, 3)), 6: ((forward_x, 5), (forward_y, 4))}.items():

        @pl.when(i == when)
        def _(todo=todo):
            for f, k in todo:
                f(k)

    wide, scale = norm_of(x_ref[...])
    a = (wide * scale).astype(BF)
    at_ref[...] = a.T
    for c, n in CH:
        g = dot(a, wgu[:, c : c + n])
        u = dot(a, wgu[:, F + c : F + c + n])
        gate_ref[:, c : c + n] = g
        up_ref[:, c : c + n] = u
        act = (g * sigmoid(g) * u).astype(BF)
        act_ref[:, c : c + n] = act
        actt_ref[c : c + n, :] = act.T

    @pl.when(i == pl.num_programs(0) - 1)
    def _():
        forward_y(5)
        for k in range(6):
            if k >= 2:
                stage_out(k).wait()
                for kind in (0, 3, 4):
                    copy(k, kind).wait_recv()
            for kind in range(5):
                copy(k, kind).wait_send()


def tile_of(tt):
    return lambda w: pl.BlockSpec((tt, w), lambda i: (i, 0))


def turned_of(tt):
    return lambda w: pl.BlockSpec((w, tt), lambda i: (0, i))


def shape(*dims, dtype=BF):
    return jax.ShapeDtypeStruct(dims, dtype)


def forward0(x, w_gate, w_up, w_down):
    tile, turned = tile_of(TT), turned_of(TT)
    return pl.pallas_call(
        k1,
        grid=(T // TT,),
        in_specs=[tile(D)] + [ANY] * 3,
        out_specs=[tile(F), tile(F), tile(F), turned(F), turned(D)] + [ANY] * 3,
        out_shape=[shape(T, F, dtype=F32)] * 2 + [shape(T, F), shape(F, T), shape(D, T), shape(2, D, F), shape(2, D, F), shape(2, F, D)],
        scratch_shapes=[
            pltpu.VMEM((D, 2 * F), BF),
            pltpu.VMEM((2, D // 4, F), BF),
            pltpu.VMEM((2, D // 4, F), BF),
            pltpu.VMEM((2, F // 4, D), BF),
            pltpu.SemaphoreType.DMA((6, 5)),
            pltpu.SemaphoreType.DMA((6, 5)),
            pltpu.SemaphoreType.DMA((6, 2)),
        ],
        compiler_params=pltpu.CompilerParams(vmem_limit_bytes=60 * 2**20, collective_id=0, has_side_effects=True),
        cost_estimate=cost(4 * T * D * F, 110e6),
        name="forward0",
    )(x, w_gate, w_up, w_down)


def k2(x_ref, act0_ref, dy_ref, wg, wu, wdn, dh_ref, at_ref, actt_ref, dgu_ref, wgu, wd, wd0, sem):
    @pl.when(pl.program_id(0) == 0)
    def _():
        copies = [
            pltpu.make_async_copy(wdn.at[0], wd0, sem.at[0]),
            pltpu.make_async_copy(wg.at[1], wgu.at[:, pl.ds(0, F)], sem.at[1]),
            pltpu.make_async_copy(wu.at[1], wgu.at[:, pl.ds(F, F)], sem.at[2]),
            pltpu.make_async_copy(wdn.at[1], wd, sem.at[3]),
        ]
        for c in copies:
            c.start()
        for c in copies:
            c.wait()

    h = (x_ref[...].astype(F32) + dot(act0_ref[...], wd0[...]).astype(BF).astype(F32)).astype(BF)
    wide, scale = norm_of(h)
    a = (wide * scale).astype(BF)
    dy = dy_ref[...]
    at_ref[...] = a.T
    for c, n in CH:
        g = dot(a, wgu[:, c : c + n])
        u = dot(a, wgu[:, F + c : F + c + n])
        dact = dot_nt(dy, wd[c : c + n, :]).astype(BF).astype(F32)
        act, dgate, dup = grads_of(g, u, dact)
        actt_ref[c : c + n, :] = act.T
        dgu_ref[:, c : c + n] = dgate
        dgu_ref[:, F + c : F + c + n] = dup
    dh_ref[...] = norm_back(dot_nt(dgu_ref[...], wgu[...]), wide, scale, dy)


def layer1(x, act0, dy, wg, wu, wd):
    tile, turned = tile_of(TT), turned_of(TT)
    return pl.pallas_call(
        k2,
        grid=(T // TT,),
        in_specs=[tile(D), tile(F), tile(D)] + [ANY] * 3,
        out_specs=[tile(D), turned(D), turned(F), tile(2 * F)],
        out_shape=[shape(T, D), shape(D, T), shape(F, T), shape(T, 2 * F)],
        scratch_shapes=[pltpu.VMEM((D, 2 * F), BF), pltpu.VMEM((F, D), BF), pltpu.VMEM((F, D), BF), pltpu.SemaphoreType.DMA((4,))],
        compiler_params=params(),
        cost_estimate=cost(12 * T * D * F, 100e6),
        name="layer1",
    )(x, act0, dy, wg, wu, wd)


def k4(dh_ref, gate_ref, up_ref, wdn, dgu_ref, wd, sem):
    @pl.when(pl.program_id(0) == 0)
    def _():
        c = pltpu.make_async_copy(wdn.at[0], wd, sem)
        c.start()
        c.wait()

    dy = dh_ref[...]
    for c, n in CH:
        dact = dot_nt(dy, wd[c : c + n, :]).astype(BF).astype(F32)
        _, dgate, dup = grads_of(gate_ref[:, c : c + n], up_ref[:, c : c + n], dact)
        dgu_ref[:, c : c + n] = dgate
        dgu_ref[:, F + c : F + c + n] = dup


def backward0(dh, gate, up, wd):
    tile = tile_of(256)
    return pl.pallas_call(
        k4,
        grid=(T // 256,),
        in_specs=[tile(D), tile(F), tile(F), ANY],
        out_specs=tile(2 * F),
        out_shape=shape(T, 2 * F),
        scratch_shapes=[pltpu.VMEM((F, D), BF), pltpu.SemaphoreType.DMA],
        compiler_params=params(),
        cost_estimate=cost(2 * T * D * F, 112e6),
        name="backward0",
    )(dh, gate, up, wd)


NA, NB, AB = 34, 12, 46
STEPS, TC = 62, 256


class Stream:
    def __init__(self, bufs, sems, slots, lags, piece_at, put):
        self.own, self.rd, self.s1, self.rx, self.s2, self.ry, self.s3, self.rz, self.s4, self.rq, self.fin = bufs
        self.send, self.recv = sems
        self.slots, self.lags, self.piece_at, self.put = slots, lags, piece_at, put

    def copies(self, c, at):
        y, low, x, core, _, partners = at
        e, n = c % 4, c % self.slots
        def make(p, src, dst, partner, slot):
            return remote(src, dst, self.send.at[p, slot], self.recv.at[p, slot], partners[partner])
        return [
            lambda: make(0, self.own.at[e, 1 - core], self.rd.at[e], CORE, e),
            lambda: make(1, self.s1.at[n, 1 - x], self.rx.at[n], X, n),
            lambda: make(2, self.s2.at[n, 1 - y], self.ry.at[n], Y, n),
            lambda: make(3, self.s3.at[n, 1 - low], self.rz.at[n], Z1, n),
            lambda: make(4, self.s4.at[n], self.rq.at[n], Z2, n),
            lambda: make(5, self.fin.at[n, y, low], self.fin.at[n, y, low], Z1, n),
            lambda: make(6, self.fin.at[n, y], self.fin.at[n, y], Y, n),
        ]

    def add(self, stage, c, at):
        y, low, x, core, _, _ = at
        e, n = c % 4, c % self.slots
        wide = lambda v: v.astype(F32)
        if stage == 1:
            self.s1[n] = (wide(self.own[e, core]) + wide(self.rd[e])).astype(BF)
        if stage == 2:
            self.s2[n] = (wide(self.s1[n, x]) + wide(self.rx[n])).astype(BF)
        if stage == 3:
            self.s3[n] = (wide(self.s2[n, y]) + wide(self.ry[n])).astype(BF)
        if stage == 4:
            self.s4[n] = (wide(self.s3[n, low]) + wide(self.rz[n])).astype(BF)
        if stage == 5:
            self.fin[n, y, low] = (wide(self.s4[n]) + wide(self.rq[n])).astype(BF)

    def advance(self, i, at):
        for stage in range(8, 0, -1):
            valid, c = self.piece_at(i - self.lags[stage])

            @pl.when(valid)
            def _(stage=stage, c=c):
                copies = self.copies(c, at)
                if stage == 8:
                    for copy in self.put(c, self.fin, c % self.slots):
                        copy.wait()
                    return
                copies[stage - 1]().wait()
                self.add(stage, c, at)
                if stage == 7:
                    for copy in self.put(c, self.fin, c % self.slots):
                        copy.start()
                else:
                    copies[stage]().start()


def piece_a(j):
    return (j >= 0) & (j < AB) & (j % 4 != 0), 3 * (j // 4) + j % 4 - 1


def piece_b(j):
    return (j >= 0) & (j < AB) & (j % 4 == 0), j // 4


LAGS_A = (0, 1, 4, 6, 8, 10, 12, 14, 15)
LAGS_B = (0, 1, 5, 8, 10, 12, 14, 16, 17)


def row_of(c):
    return pl.multiple_of(jnp.minimum(c % 6 * 96, 448), 32)


def k5(dgu1_ref, dgu0_ref, x_ref, dht_ref, tile_ref, dy, dh, at1, at0, actt1, actt0, wg, wu, dx_ref, out_gu, out_d, *rest):
    abufs, bbufs, rest = rest[:11], rest[11:22], rest[22:]
    (asend, arecv, bsend, brecv, aput, bput, big0, big1, lt1, lt0, lhs, wgu, sem, lsem) = rest
    i = pl.program_id(0)
    at = places()

    def put_a(c, fin, n):
        where = out_gu.at[1 - c // 17, :, :, :, pl.ds(pl.multiple_of(c % 17 * 256, 256), 256)]
        return [pltpu.make_async_copy(fin.at[n], where, aput.at[n])]

    def put_b(c, fin, n):
        row = row_of(c)
        return [pltpu.make_async_copy(fin.at[n, q // 2, q % 2], out_d.at[1 - c // 6, pl.ds(pl.multiple_of(row + 24 * q, 8), 24)], bput.at[n, q]) for q in range(4)]

    a = Stream(abufs, (asend, arecv), 6, LAGS_A, piece_a, put_a)
    b = Stream(bbufs, (bsend, brecv), 4, LAGS_B, piece_b, put_b)

    load = [
        pltpu.make_async_copy(dy, big1, sem.at[0]),
        pltpu.make_async_copy(at1, lt1, sem.at[1]),
        pltpu.make_async_copy(at0, lt0, sem.at[2]),
        pltpu.make_async_copy(dh, big0, sem.at[3]),
        pltpu.make_async_copy(wg.at[0], wgu.at[:, pl.ds(0, F)], sem.at[4]),
        pltpu.make_async_copy(wu.at[0], wgu.at[:, pl.ds(F, F)], sem.at[5]),
    ]

    def lhs_copies(c, source):
        row = row_of(c)
        return [pltpu.make_async_copy(source.at[pl.ds(pl.multiple_of(544 * q + row, 32), 96)], lhs.at[c % 2, pl.ds(96 * q, 96)], lsem.at[c % 2, q]) for q in range(4)]

    def fetch_lhs(c):
        @pl.when(c < 6)
        def _():
            for copy in lhs_copies(c, actt1):
                copy.start()

        @pl.when((c >= 6) & (c < NB))
        def _():
            for copy in lhs_copies(c, actt0):
                copy.start()

    @pl.when(i == 0)
    def _():
        fetch_lhs(0 * i)
        for copy in load:
            copy.start()
        greet(at[5])
        load[0].wait()

    for when, which in {1: (1,), 23: (2,), 24: (3,), AB: (4, 5)}.items():

        @pl.when(i == when)
        def _(which=which):
            for w in which:
                load[w].wait()

    a.advance(i, at)
    b.advance(i, at)

    is_a, ca = piece_a(i)
    is_b, cb = piece_b(i)

    def weight_a(lt, r):
        out = dot(lt[...], r[...])
        for q in range(4):
            a.own[ca % 4, q % 2, q // 2] = out[160 * q : 160 * q + 160].reshape(2, 2, 40, 256).astype(BF)
        a.copies(ca, at)[0]().start()

    def weight_b(big):
        for copy in lhs_copies(cb, actt1):
            copy.wait()
        fetch_lhs(cb + 1)
        out = dot(lhs[cb % 2], big[...])
        for q in range(4):
            b.own[cb % 4, q % 2, q // 2] = out[96 * q : 96 * q + 96].reshape(2, 2, 24, D).astype(BF)
        b.copies(cb, at)[0]().start()

    pl.when(is_a & (ca < 17))(lambda: weight_a(lt1, dgu1_ref))
    pl.when(is_a & (ca >= 17))(lambda: weight_a(lt0, dgu0_ref))
    pl.when(is_b & (cb < 6))(lambda: weight_b(big1))
    pl.when(is_b & (cb >= 6))(lambda: weight_b(big0))

    @pl.when(i >= AB)
    def _():
        wide, scale = norm_of(x_ref[...])
        dx_ref[...] = norm_back(dot_nt(tile_ref[...], wgu[...]), wide, scale, dht_ref[...])


def weights_and_input(x, dy, dh, at1, at0, actt1, actt0, dgu1, dgu0, wg, wu):
    def piece(first):
        def index(i):
            j = jnp.minimum(i, AB - 1)
            return (0, jnp.clip(3 * (j // 4) + jnp.maximum(j % 4 - 1, 0) - first, 0, 16))
        return index
    tile = lambda w: pl.BlockSpec((TC, w), lambda i: (jnp.maximum(i - AB, 0), 0))

    def bufs(own_slots, n, r, c):
        v = lambda *dims: pltpu.VMEM(dims + (r, c), BF)
        return [v(4, 2, 2, 2, 2), v(4, 2, 2, 2), v(n, 2, 2, 2), v(n, 2, 2), v(n, 2, 2), v(n, 2), v(n, 2), v(n), v(n), v(n), v(n, 2, 2)]

    dma = pltpu.SemaphoreType.DMA
    return pl.pallas_call(
        k5,
        grid=(STEPS,),
        in_specs=[pl.BlockSpec((T, 256), piece(0)), pl.BlockSpec((T, 256), piece(17)), tile(D), tile(D), tile(2 * F)] + [ANY] * 8,
        out_specs=[tile(D), ANY, ANY],
        out_shape=[shape(T, D), shape(2, 2, 2, 40, 2 * F), shape(2, F // 4, D)],
        scratch_shapes=bufs(4, 6, 40, 256)
        + bufs(4, 4, 24, D)
        + [dma((7, 6)), dma((7, 6)), dma((7, 4)), dma((7, 4)), dma((6,)), dma((4, 4))]
        + [pltpu.VMEM((T, D), BF), pltpu.VMEM((T, D), BF), pltpu.VMEM((D, T), BF), pltpu.VMEM((D, T), BF)]
        + [pltpu.VMEM((2, 384, T), BF), pltpu.VMEM((D, 2 * F), BF), dma((6,)), dma((2, 4))],
        compiler_params=pltpu.CompilerParams(vmem_limit_bytes=67043328, collective_id=1, has_side_effects=True),
        cost_estimate=cost(16 * T * D * F, 150e6),
        name="weights_and_input",
    )(dgu1, dgu0, x, dh, dgu0, dy, dh, at1, at0, actt1, actt0, wg, wu)


def solution(mesh):
    def step(x, dy, w_gate, w_up, w_down):
        x, dy = x[0], dy[0]
        gate, up, act0, actt0, at0, wg, wu, wd = forward0(x, w_gate, w_up, w_down)
        dh, at1, actt1, dgu1 = layer1(x, act0, dy, wg, wu, wd)
        dgu0 = backward0(dh, gate, up, wd)
        dx, gu, down = weights_and_input(x, dy, dh, at1, at0, actt1, actt0, dgu1, dgu0, wg, wu)
        gu = gu.reshape(2, D // 4, 2 * F)
        return dx[None], gu[:, :, :F], gu[:, :, F:], down

    states, cut = P(("rep", "r", "s"), None, None), P(None, "s", None)
    return jax.shard_map(
        step,
        mesh=mesh,
        in_specs=(states, states) + (cut,) * 3,
        out_specs=(states,) + (P("rep", "s", None),) * 3,
        check_vma=False,
    )
```

```python
import functools
import jax
import jax.numpy as jnp
from jax import lax
from jax.experimental import pallas as pl
from jax.experimental.pallas import tpu as pltpu
from jax.sharding import PartitionSpec as P

T, D, F, EPS = 4096, 640, 2176, 1e-6
BF, F32 = jnp.bfloat16, jnp.float32
TT = 512
CH = [(i * 256, 256) for i in range(8)] + [(2048, 128)]
ANY = pl.BlockSpec(memory_space=pl.ANY)
NT = (((1,), (1,)), ((), ()))


def dot(a, b):
    return jnp.dot(a, b, preferred_element_type=F32)


def dot_nt(a, b):
    return lax.dot_general(a, b, NT, preferred_element_type=F32)


def params(limit=60):
    return pltpu.CompilerParams(vmem_limit_bytes=limit * 2**20)


def cost(flops, nbytes):
    return pl.CostEstimate(flops=int(flops), bytes_accessed=int(nbytes), transcendentals=0)


def norm_of(h):
    wide = h.astype(F32)
    scale = lax.rsqrt(jnp.mean(wide * wide, -1, keepdims=True) + EPS)
    return wide, scale


def sigmoid(g):
    return 1.0 / (1.0 + jnp.exp(-g))


def grads_of(g, u, dact):
    sig = sigmoid(g)
    silu = g * sig
    act = (silu * u).astype(BF)
    dup = dact * silu
    dgate = dact * u * (sig + silu * (1.0 - sig))
    return act, dgate.astype(BF), dup.astype(BF)


def norm_back(da, wide, scale, dy):
    da = da.astype(BF).astype(F32)
    inner = jnp.mean(da * wide, -1, keepdims=True)
    dwide = scale * da - wide * (scale * scale * scale * inner)
    return (dy.astype(F32) + dwide.astype(BF).astype(F32)).astype(BF)


CORE, X, Z1, Z2, Y = range(5)
MESH = pl.DeviceIdType.MESH


def places():
    rep, r, s = lax.axis_index("rep"), lax.axis_index("r"), lax.axis_index("s")
    y, z, x, core = r // 4, r % 4, s // 2, s % 2
    at = lambda y, z, x, core: (rep, y * 4 + z, x * 2 + core)
    low, high = z % 2, z // 2
    partners = [
        at(y, z, x, 1 - core),
        at(y, z, 1 - x, core),
        at(y, high * 2 + 1 - low, x, core),
        at(y, (1 - high) * 2 + low, x, core),
        at(1 - y, z, x, core),
    ]
    return y, low, x, core, s, partners


def greet(partners):
    barrier = pltpu.get_barrier_semaphore()
    for partner in partners:
        pl.semaphore_signal(barrier, inc=1, device_id=partner, device_id_type=MESH)
    pl.semaphore_wait(barrier, len(partners))


def remote(src, dst, send, recv, partner):
    return pltpu.make_async_remote_copy(src_ref=src, dst_ref=dst, send_sem=send, recv_sem=recv, device_id=partner, device_id_type=MESH)


def k1(x_ref, wg, wu, wd, gate_ref, up_ref, act_ref, actt_ref, at_ref, og, ou, od, wgu, sg, su, sd, send, recv, local):
    i = pl.program_id(0)
    y, low, x, core, s, partners = places()
    tensors = [(w, o, stage, layer, rows) for layer in range(2) for w, o, stage, rows in ((wg, og, sg, 160), (wu, ou, su, 160), (wd, od, sd, 544))]

    def copy(k, kind):
        w, o, _, layer, rows = tensors[k]
        half = rows // 2
        across = jnp.bitwise_xor(s, 2)
        own = lambda n, at: o.at[layer, pl.ds(pl.multiple_of(at, 16), n)]
        if kind == 0:
            src, dst, partner = w.at[layer], own(rows, s * rows), CORE
        elif kind == 1:
            src, dst, partner = w.at[layer, pl.ds(pl.multiple_of(y * half, 16), half)], own(half, s * rows + y * half), X
        elif kind in (2, 3):
            src = own(half, across * rows + y * half)
            dst, partner = src, Y if kind == 2 else CORE
        else:
            src = own(half, across * rows + (1 - y) * half)
            dst, partner = src, CORE
        return remote(src, dst, send.at[k, kind], recv.at[k, kind], partners[partner])

    def stage_in(k):
        w, _, stage, layer, _ = tensors[k]
        return pltpu.make_async_copy(w.at[layer], stage.at[layer], local.at[k, 0])

    def stage_out(k):
        _, o, stage, layer, rows = tensors[k]
        return pltpu.make_async_copy(stage.at[layer], o.at[layer, pl.ds(pl.multiple_of(s * rows, 32), rows)], local.at[k, 1])

    def forward_x(k):
        copy(k, 1).wait_recv()
        copy(k, 2).start()
        copy(k, 3).start()

    def forward_y(k):
        copy(k, 2).wait_recv()
        copy(k, 4).start()

    @pl.when(i == 0)
    def _():
        greet([partners[CORE], partners[X], partners[Y]])
        copy(0, 1).start()
        copy(1, 1).start()
        copy(0, 0).start()
        copy(1, 0).start()
        for k in range(6):
            stage_in(k).start()
        for k in range(6):
            stage_in(k).wait()
            stage_out(k).start()
        forward_x(0)
        copy(2, 1).start()
        forward_x(1)
        for k in range(3, 6):
            copy(k, 1).start()
        forward_y(0)
        forward_y(1)
        for k in range(2):
            stage_out(k).wait()
            for kind in (0, 3, 4):
                copy(k, kind).wait_recv()
        loads = [pltpu.make_async_copy(o.at[0], wgu.at[:, pl.ds(c, F)], local.at[c // F, 0]) for o, c in ((og, 0), (ou, F))]
        for load in loads:
            load.start()
        for k in range(2, 6):
            copy(k, 0).start()
        for load in loads:
            load.wait()

    for when, todo in {1: ((forward_x, 2),), 3: ((forward_x, 3), (forward_y, 2)), 4: ((forward_x, 4), (forward_y, 3)), 6: ((forward_x, 5), (forward_y, 4))}.items():

        @pl.when(i == when)
        def _(todo=todo):
            for f, k in todo:
                f(k)

    wide, scale = norm_of(x_ref[...])
    a = (wide * scale).astype(BF)
    at_ref[...] = a.T
    for c, n in CH:
        g = dot(a, wgu[:, c : c + n])
        u = dot(a, wgu[:, F + c : F + c + n])
        gate_ref[:, c : c + n] = g
        up_ref[:, c : c + n] = u
        act = (g * sigmoid(g) * u).astype(BF)
        act_ref[:, c : c + n] = act
        actt_ref[c : c + n, :] = act.T

    @pl.when(i == pl.num_programs(0) - 1)
    def _():
        forward_y(5)
        for k in range(6):
            if k >= 2:
                stage_out(k).wait()
                for kind in (0, 3, 4):
                    copy(k, kind).wait_recv()
            for kind in range(5):
                copy(k, kind).wait_send()


def tile_of(tt):
    return lambda w: pl.BlockSpec((tt, w), lambda i: (i, 0))


def turned_of(tt):
    return lambda w: pl.BlockSpec((w, tt), lambda i: (0, i))


def shape(*dims, dtype=BF):
    return jax.ShapeDtypeStruct(dims, dtype)


def forward0(x, w_gate, w_up, w_down):
    tile, turned = tile_of(TT), turned_of(TT)
    return pl.pallas_call(
        k1,
        grid=(T // TT,),
        in_specs=[tile(D)] + [ANY] * 3,
        out_specs=[tile(F), tile(F), tile(F), turned(F), turned(D)] + [ANY] * 3,
        out_shape=[shape(T, F, dtype=F32)] * 2 + [shape(T, F), shape(F, T), shape(D, T), shape(2, D, F), shape(2, D, F), shape(2, F, D)],
        scratch_shapes=[
            pltpu.VMEM((D, 2 * F), BF),
            pltpu.VMEM((2, D // 4, F), BF),
            pltpu.VMEM((2, D // 4, F), BF),
            pltpu.VMEM((2, F // 4, D), BF),
            pltpu.SemaphoreType.DMA((6, 5)),
            pltpu.SemaphoreType.DMA((6, 5)),
            pltpu.SemaphoreType.DMA((6, 2)),
        ],
        compiler_params=pltpu.CompilerParams(vmem_limit_bytes=60 * 2**20, collective_id=0, has_side_effects=True),
        cost_estimate=cost(4 * T * D * F, 110e6),
        name="forward0",
    )(x, w_gate, w_up, w_down)


def k2(x_ref, act0_ref, dy_ref, wg, wu, wdn, dh_ref, at_ref, actt_ref, dgu_ref, wgu, wd, wd0, sem):
    @pl.when(pl.program_id(0) == 0)
    def _():
        copies = [
            pltpu.make_async_copy(wdn.at[0], wd0, sem.at[0]),
            pltpu.make_async_copy(wg.at[1], wgu.at[:, pl.ds(0, F)], sem.at[1]),
            pltpu.make_async_copy(wu.at[1], wgu.at[:, pl.ds(F, F)], sem.at[2]),
            pltpu.make_async_copy(wdn.at[1], wd, sem.at[3]),
        ]
        for c in copies:
            c.start()
        for c in copies:
            c.wait()

    parts = []
    for r in range(0, TT, 256):
        h = (x_ref[r : r + 256, :].astype(F32) + dot(act0_ref[r : r + 256, :], wd0[...]).astype(BF).astype(F32)).astype(BF)
        parts.append((*norm_of(h),))
    wide, scale = (jnp.concatenate(p, 0) for p in zip(*parts))
    a = (wide * scale).astype(BF)
    dy = dy_ref[...]
    at_ref[...] = a.T
    for c, n in CH:
        g = dot(a, wgu[:, c : c + n])
        u = dot(a, wgu[:, F + c : F + c + n])
        dact = dot_nt(dy, wd[c : c + n, :]).astype(BF).astype(F32)
        act, dgate, dup = grads_of(g, u, dact)
        actt_ref[c : c + n, :] = act.T
        dgu_ref[:, c : c + n] = dgate
        dgu_ref[:, F + c : F + c + n] = dup
    for r in range(0, TT, 256):
        q = slice(r, r + 256)
        dh_ref[q, :] = norm_back(dot_nt(wgu[...], dgu_ref[q, :]).T, wide[q], scale[q], dy[q])


def layer1(x, act0, dy, wg, wu, wd):
    tile, turned = tile_of(TT), turned_of(TT)
    return pl.pallas_call(
        k2,
        grid=(T // TT,),
        in_specs=[tile(D), tile(F), tile(D)] + [ANY] * 3,
        out_specs=[tile(D), turned(D), turned(F), tile(2 * F)],
        out_shape=[shape(T, D), shape(D, T), shape(F, T), shape(T, 2 * F)],
        scratch_shapes=[pltpu.VMEM((D, 2 * F), BF), pltpu.VMEM((F, D), BF), pltpu.VMEM((F, D), BF), pltpu.SemaphoreType.DMA((4,))],
        compiler_params=params(),
        cost_estimate=cost(12 * T * D * F, 100e6),
        name="layer1",
    )(x, act0, dy, wg, wu, wd)


def k4(dh_ref, gate_ref, up_ref, wdn, dgu_ref, wd, sem):
    @pl.when(pl.program_id(0) == 0)
    def _():
        c = pltpu.make_async_copy(wdn.at[0], wd, sem)
        c.start()
        c.wait()

    dy = dh_ref[...]
    for c, n in CH:
        dact = dot_nt(dy, wd[c : c + n, :]).astype(BF).astype(F32)
        _, dgate, dup = grads_of(gate_ref[:, c : c + n], up_ref[:, c : c + n], dact)
        dgu_ref[:, c : c + n] = dgate
        dgu_ref[:, F + c : F + c + n] = dup


def backward0(dh, gate, up, wd):
    tile = tile_of(512)
    return pl.pallas_call(
        k4,
        grid=(T // 512,),
        in_specs=[tile(D), tile(F), tile(F), ANY],
        out_specs=tile(2 * F),
        out_shape=shape(T, 2 * F),
        scratch_shapes=[pltpu.VMEM((F, D), BF), pltpu.SemaphoreType.DMA],
        compiler_params=params(),
        cost_estimate=cost(2 * T * D * F, 112e6),
        name="backward0",
    )(dh, gate, up, wd)


PAIRS, NB, CYCLES = 17, 12, 17
STEPS, TC = 62, 256
MIX = 3 * CYCLES
EARLY = CYCLES - NB


class Stream:
    def __init__(self, bufs, sems, count, first, put):
        self.own, self.rd, self.s1, self.rx, self.s2, self.ry, self.s3, self.rz, self.s4, self.rq, self.fin = bufs
        self.send, self.recv = sems
        self.count, self.first, self.put = count, first, put

    def copies(self, c, at):
        y, low, x, core, _, partners = at
        e, n = c & 1, c & 3

        def make(p, src, dst, partner, slot):
            return remote(src, dst, self.send.at[p, slot], self.recv.at[p, slot], partners[partner])

        return [
            lambda: make(0, self.own.at[e, 1 - core], self.rd.at[e], CORE, e),
            lambda: make(1, self.s1.at[n, 1 - x], self.rx.at[n], X, n),
            lambda: make(2, self.s2.at[n, 1 - y], self.ry.at[n], Y, n),
            lambda: make(3, self.s3.at[n, 1 - low], self.rz.at[n], Z1, n),
            lambda: make(4, self.s4.at[n], self.rq.at[n], Z2, n),
            lambda: make(5, self.fin.at[n, y, low], self.fin.at[n, y, low], Z1, n),
            lambda: make(6, self.fin.at[n, y], self.fin.at[n, y], Y, n),
        ]

    def add(self, stage, c, at):
        y, low, x, core, _, _ = at
        e, n = c & 1, c & 3
        wide = lambda v: v.astype(F32)
        if stage == 1:
            self.s1[n] = (wide(self.own[e, core]) + wide(self.rd[e])).astype(BF)
        if stage == 2:
            self.s2[n] = (wide(self.s1[n, x]) + wide(self.rx[n])).astype(BF)
        if stage == 3:
            self.s3[n] = (wide(self.s2[n, y]) + wide(self.ry[n])).astype(BF)
        if stage == 4:
            self.s4[n] = (wide(self.s3[n, low]) + wide(self.rz[n])).astype(BF)
        if stage == 5:
            self.fin[n, y, low] = (wide(self.s4[n]) + wide(self.rq[n])).astype(BF)

    def advance(self, cycle, at):
        for stage in range(8, 0, -1):
            c = cycle - stage + self.first

            @pl.when((c >= 0) & (c < self.count))
            def _(stage=stage, c=c):
                copies = self.copies(c, at)
                if stage == 8:
                    for copy in self.put(c, self.fin, c & 3):
                        copy.wait()
                    return
                copies[stage - 1]().wait()
                self.add(stage, c, at)
                if stage == 7:
                    for copy in self.put(c, self.fin, c & 3):
                        copy.start()
                else:
                    copies[stage]().start()


def row_of(c):
    return pl.multiple_of(jnp.minimum((c - jnp.where(c >= 6, 6, 0)) * 96, 448), 32)


def k5(dgu1_ref, dgu0_ref, x_ref, dht_ref, tile_ref, dy, dh, at1, at0, actt1, actt0, wg, wu, dx_ref, out_gu, out_d, *rest):
    abufs, bbufs, rest = rest[:11], rest[11:22], rest[22:]
    (asend, arecv, bsend, brecv, aput, bput, big0, big1, lt1, lt0, lhs, wgu, sem, lsem) = rest
    i = pl.program_id(0)
    at = places()

    def put_a(c, fin, n):
        copies = []
        for half in range(2):
            part = 2 * c + half
            late = jnp.where(part >= 17, 1, 0)
            where = out_gu.at[1 - late, :, :, :, pl.ds(pl.multiple_of((part - 17 * late) * 256, 256), 256)]
            copies.append(pltpu.make_async_copy(fin.at[n, :, :, :, pl.ds(256 * half, 256)], where, aput.at[n, half]))
        return copies

    def put_b(c, fin, n):
        row = row_of(c)
        return [pltpu.make_async_copy(fin.at[n, q // 2, q % 2], out_d.at[jnp.where(c >= 6, 0, 1), pl.ds(pl.multiple_of(row + 24 * q, 8), 24)], bput.at[n, q]) for q in range(4)]

    a = Stream(abufs, (asend, arecv), PAIRS, 0, put_a)
    b = Stream(bbufs, (bsend, brecv), NB, 1, put_b)

    load = [
        pltpu.make_async_copy(dy, big1, sem.at[0]),
        pltpu.make_async_copy(at1, lt1, sem.at[1]),
        pltpu.make_async_copy(at0, lt0, sem.at[2]),
        pltpu.make_async_copy(dh, big0, sem.at[3]),
        pltpu.make_async_copy(wg.at[0], wgu.at[:, pl.ds(0, F)], sem.at[4]),
        pltpu.make_async_copy(wu.at[0], wgu.at[:, pl.ds(F, F)], sem.at[5]),
    ]

    def lhs_copies(c, source):
        row = row_of(c)
        return [pltpu.make_async_copy(source.at[pl.ds(pl.multiple_of(544 * q + row, 32), 96)], lhs.at[c & 1, pl.ds(96 * q, 96)], lsem.at[c & 1, q]) for q in range(4)]

    def fetch_lhs(c):
        @pl.when(c < 6)
        def _():
            for copy in lhs_copies(c, actt1):
                copy.start()

        @pl.when((c >= 6) & (c < NB))
        def _():
            for copy in lhs_copies(c, actt0):
                copy.start()

    @pl.when(i == 0)
    def _():
        fetch_lhs(0 * i)
        for copy in load:
            copy.start()
        greet(at[5])
        load[0].wait()

    for when, which in {1: (1,), 18: (3,), 26: (2,), 3 * NB: (4, 5)}.items():

        @pl.when(i == when)
        def _(which=which):
            for w in which:
                load[w].wait()

    cycle = lax.div(i, 3)
    place = i - 3 * cycle
    mixed = i < MIX
    tick = jnp.where(mixed, cycle, i - MIX + CYCLES)
    pl.when(~mixed | (place == 1))(lambda: a.advance(tick, at))
    pl.when(~mixed | (place == 2))(lambda: b.advance(tick, at))

    is_a, ca = mixed & (place > 0), 2 * cycle + place - 1
    is_b, cb = mixed & (place == 0) & (cycle < NB), cycle

    def weight_a(lt, r):
        out = dot(lt[...], r[...])
        pair, half = cycle, place - 1
        for q in range(4):
            part = out[160 * q : 160 * q + 160].reshape(2, 2, 40, 256).astype(BF)
            a.own[pair & 1, q % 2, q // 2, :, :, :, pl.ds(pl.multiple_of(half * 256, 256), 256)] = part

        @pl.when(half == 1)
        def _():
            a.copies(pair, at)[0]().start()

    def weight_b(big):
        for copy in lhs_copies(cb, actt1):
            copy.wait()
        fetch_lhs(cb + 1)
        out = dot(lhs[cb & 1], big[...])
        for q in range(4):
            b.own[cb & 1, q % 2, q // 2] = out[96 * q : 96 * q + 96].reshape(2, 2, 24, D).astype(BF)
        b.copies(cb, at)[0]().start()

    pl.when(is_a & (ca < 17))(lambda: weight_a(lt1, dgu1_ref))
    pl.when(is_a & (ca >= 17))(lambda: weight_a(lt0, dgu0_ref))
    pl.when(is_b & (cb < 6))(lambda: weight_b(big1))
    pl.when(is_b & (cb >= 6))(lambda: weight_b(big0))

    @pl.when(~mixed | ((place == 0) & (cycle >= NB)))
    def _():
        wide, scale = norm_of(x_ref[...])
        dx_ref[...] = norm_back(dot_nt(wgu[...], tile_ref[...]).T, wide, scale, dht_ref[...])


def weights_and_input(x, dy, dh, at1, at0, actt1, actt0, dgu1, dgu0, wg, wu):
    def piece(first):
        def index(i):
            j = jnp.minimum(i, MIX - 1)
            part = 2 * (j // 3) + jnp.maximum(j % 3 - 1, 0)
            return (0, jnp.clip(part - first, 0, 16))

        return index

    def index(i):
        return (jnp.where(i < MIX, jnp.clip(i // 3 - NB, 0, EARLY - 1), i - MIX + EARLY), 0)

    tile = lambda w: pl.BlockSpec((TC, w), index)

    def bufs(n, r, c):
        v = lambda *dims: pltpu.VMEM(dims + (r, c), BF)
        return [v(2, 2, 2, 2, 2), v(2, 2, 2, 2), v(n, 2, 2, 2), v(n, 2, 2), v(n, 2, 2), v(n, 2), v(n, 2), v(n), v(n), v(n), v(n, 2, 2)]

    dma = pltpu.SemaphoreType.DMA
    return pl.pallas_call(
        k5,
        grid=(STEPS,),
        in_specs=[pl.BlockSpec((T, 256), piece(0)), pl.BlockSpec((T, 256), piece(17)), tile(D), tile(D), tile(2 * F)] + [ANY] * 8,
        out_specs=[tile(D), ANY, ANY],
        out_shape=[shape(T, D), shape(2, 2, 2, 40, 2 * F), shape(2, F // 4, D)],
        scratch_shapes=bufs(4, 40, 512)
        + bufs(4, 24, D)
        + [dma((7, 4)), dma((7, 4)), dma((7, 4)), dma((7, 4)), dma((4, 2)), dma((4, 4))]
        + [pltpu.VMEM((T, D), BF), pltpu.VMEM((T, D), BF), pltpu.VMEM((D, T), BF), pltpu.VMEM((D, T), BF)]
        + [pltpu.VMEM((2, 384, T), BF), pltpu.VMEM((D, 2 * F), BF), dma((6,)), dma((2, 4))],
        compiler_params=pltpu.CompilerParams(vmem_limit_bytes=67043328, collective_id=1, has_side_effects=True),
        cost_estimate=cost(16 * T * D * F, 150e6),
        name="weights_and_input",
    )(dgu1, dgu0, x, dh, dgu0, dy, dh, at1, at0, actt1, actt0, wg, wu)


def solution(mesh):
    def step(x, dy, w_gate, w_up, w_down):
        x, dy = x[0], dy[0]
        gate, up, act0, actt0, at0, wg, wu, wd = forward0(x, w_gate, w_up, w_down)
        dh, at1, actt1, dgu1 = layer1(x, act0, dy, wg, wu, wd)
        dgu0 = backward0(dh, gate, up, wd)
        dx, gu, down = weights_and_input(x, dy, dh, at1, at0, actt1, actt0, dgu1, dgu0, wg, wu)
        gu = gu.reshape(2, D // 4, 2 * F)
        return dx[None], gu[:, :, :F], gu[:, :, F:], down

    states, cut = P(("rep", "r", "s"), None, None), P(None, "s", None)
    return jax.shard_map(
        step,
        mesh=mesh,
        in_specs=(states, states) + (cut,) * 3,
        out_specs=(states,) + (P("rep", "s", None),) * 3,
        check_vma=False,
    )
```
